32 devices in a mesh: seq: 8 (over z, y), head: 4 (over x, core).
Axes of the slice: x: 2, y: 2, z: 4, core: 2. Of those that a mesh axis runs over, the one named last changes fastest.
Arguments:
- queries: bfloat16 [4096, 2048], P('seq', 'head'), may hold values from -6 to 6
- keys: bfloat16 [4096, 2048], P('seq', 'head'), may hold values from -6 to 6
- values: bfloat16 [4096, 4096], P('seq', 'head'), may hold values from -6 to 6
- forget_gate: float32 [4096, 8], P('seq', 'head'), may hold values from -1 to 14
- input_gate: float32 [4096, 8], P('seq', 'head'), may hold values from -5 to 215
- out_weight: bfloat16 [4096, 4096], P('head'), may hold values from -0.125 to 0.125
Outputs:
- mixed: bfloat16 [4096, 4096], P('seq', 'head')
- gate_mean: float32 [8], P('head')
The draws below stay inside these ranges and needn't reach their ends.
All inputs are finite; a program needn't handle non-finite values.
Results may differ from the reference program's by a relative error of at most 0.01.
Values may be sent and summed in bfloat16 or wider, within the bound.
A program may use at most 192 MiB of HBM per device.

```python
import math
import jax
import jax.numpy as jnp
from jax import lax

D = 4096
HEAD_TOTAL = 8
DQK = 256
DV = 512
TOK_DEV = 512
SEQUENCE_TOKENS = 4096
N_HEAD = 4


def draw_forget_gate(key, part):
    starting_key = jax.random.fold_in(key, 101)
    key_for_shuffle, key_for_token, key_for_block, key_for_spike, key_magnitude = jax.random.split(starting_key, 5)
    head_order = jax.random.permutation(key_for_shuffle, HEAD_TOTAL)
    keep_count = HEAD_TOTAL // 2
    slow_heads = head_order < keep_count
    starting_rate = jnp.where(slow_heads, math.log(10.0) / (4.0 * SEQUENCE_TOKENS), 1.0 / 40.0).astype(jnp.float32)
    token_multiplier = jnp.exp(jax.random.uniform(key_for_token, (SEQUENCE_TOKENS, HEAD_TOTAL), jnp.float32, -0.6931, 0.6931))
    block_count = SEQUENCE_TOKENS // TOK_DEV
    block_multiplier = jnp.exp(jax.random.uniform(key_for_block, (block_count, HEAD_TOTAL), jnp.float32, -0.6931, 0.6931))
    block_multiplier = jnp.repeat(block_multiplier, TOK_DEV, axis=0)
    spike_mask = jax.random.uniform(key_for_spike, (SEQUENCE_TOKENS, HEAD_TOTAL), jnp.float32) < 3.0 / SEQUENCE_TOKENS
    spike_magnitude = jax.random.uniform(key_magnitude, (SEQUENCE_TOKENS, HEAD_TOTAL), jnp.float32, 0.2231, 0.6931)
    forget_rate = starting_rate[None, :] * token_multiplier * block_multiplier + jnp.where(spike_mask, spike_magnitude, 0.0)
    return (-jnp.log(jnp.expm1(forget_rate))).astype(jnp.float32)


def draw_input_gate(key, part):
    starting_key = jax.random.fold_in(key, 202)
    key_noise = jax.random.fold_in(starting_key, 0)
    position_ramp = (jnp.arange(SEQUENCE_TOKENS).astype(jnp.float32) / SEQUENCE_TOKENS)[:, None]
    jitter = jnp.clip(jax.random.normal(key_noise, (SEQUENCE_TOKENS, HEAD_TOTAL), jnp.float32), -4.0, 4.0)
    result = 1.0 + 2.0 * position_ramp + jitter
    return result.astype(jnp.float32)


def with_spikes(array, own_key, source, target, blocks, factor):
    def block_of(dim):
        return (jnp.arange(array.shape[dim]) // (array.shape[dim] // blocks)).reshape((-1,) + (1,) * (array.ndim - 1 - dim))

    near = jax.random.permutation(own_key, blocks)[block_of(target)]
    other_side = (block_of(target) + blocks // 2) % blocks
    return jnp.where((block_of(source) == near) | (block_of(source) == other_side), factor * array, array)


def levels(key, dims, cuts, smallest, largest):
    level, own = 1.0, jax.random.fold_in(key, 6)
    for position, blocks in cuts:
        steps = jnp.exp(jax.random.uniform(jax.random.fold_in(own, position), (blocks,), jnp.float32, smallest / len(cuts), largest / len(cuts)))
        level = level * jnp.repeat(steps, dims[position] // blocks).reshape([-1 if axis == position else 1 for axis in range(len(dims))])
    return level


def bell_draw(key, dims, scale, reach, shards=(), kind=jnp.bfloat16):
    drawn = jax.random.normal(key, dims, jnp.float32) * scale
    if len(shards) > 0:
        drawn = levels(key, dims, shards, -0.22, 0.18) * drawn
    return jnp.clip(drawn, min=-reach, max=reach).astype(kind)


def gaussian_with(rng, dims, width, most, cuts, heavy, kind=jnp.bfloat16):
    values = width * jax.random.normal(rng, dims, jnp.float32)
    if cuts:
        values = values * levels(rng, dims, cuts, -0.22, 0.18)
    return jnp.clip(with_spikes(values, jax.random.fold_in(rng, 3), *heavy), -most, most).astype(kind)


def setup_inputs(seed: int = 0) -> dict:
    splits = jax.random.split(jax.random.key(seed), 7)
    return {
        "queries": bell_draw(splits[0], (SEQUENCE_TOKENS, HEAD_TOTAL * DQK), 1.0, 6.0, ((0, 8), (1, 4))),
        "keys": bell_draw(splits[1], (SEQUENCE_TOKENS, HEAD_TOTAL * DQK), 1.0, 6.0, ((0, 8), (1, 4))),
        "values": bell_draw(splits[2], (SEQUENCE_TOKENS, HEAD_TOTAL * DV), 1.0, 6.0, ((0, 8), (1, 4))),
        "forget_gate": draw_forget_gate(jax.random.fold_in(splits[6], 71), 0),
        "input_gate": draw_input_gate(jax.random.fold_in(splits[6], 71), 0),
        "out_weight": gaussian_with(splits[5], (HEAD_TOTAL * DV, D), (HEAD_TOTAL * DV) ** -0.5, 0.125, ((0, 4),), (0, 1, 4, 2.0)),
    }


def combine_states(earlier, later_state):
    e_matrix, e_norm, e_max, e_decay = earlier
    l_matrix, l_norm, l_max, l_decay = later_state
    merged_max = jnp.maximum(l_decay + e_max, l_max)
    e_scale = jnp.exp(l_decay + e_max - merged_max)
    l_scale = jnp.exp(l_max - merged_max)
    return (e_scale[:, None, None] * e_matrix + l_scale[:, None, None] * l_matrix, e_scale[:, None] * e_norm + l_scale[:, None] * l_norm, merged_max, e_decay + l_decay)

def intra_terms(q_heads, k_heads, v_heads, cum_decay, input_block):
    length = q_heads.shape[0]
    positions = jnp.arange(length)
    causal = positions[:, None] >= positions[None, :]
    log_weight = cum_decay.T[:, :, None] - cum_decay.T[:, None, :] + input_block.T[:, None, :]
    log_weight = jnp.where(causal[None], log_weight, -jnp.inf)
    intra_max = lax.optimization_barrier(jnp.max(log_weight, axis=2))
    factors = jnp.exp(log_weight - intra_max[:, :, None])
    scores = jnp.einsum('thd,shd->hts', q_heads.astype(jnp.float32), k_heads.astype(jnp.float32)) / math.sqrt(q_heads.shape[2])
    weighted = factors * scores
    intra_den = lax.optimization_barrier(jnp.sum(weighted, axis=2))
    rounded_weights = lax.optimization_barrier(weighted.astype(jnp.bfloat16))
    intra_num = jnp.einsum('hts,shv->thv', rounded_weights.astype(jnp.float32), v_heads.astype(jnp.float32))
    return (intra_num, intra_den, intra_max)

def own_terms(k_heads, v_heads, cum_decay, input_block):
    block_decay = cum_decay[-1]
    own_log = block_decay[None, :] - cum_decay + input_block
    own_max = lax.optimization_barrier(jnp.max(own_log, axis=0))
    key_weight = jnp.exp(own_log - own_max[None, :]) / math.sqrt(k_heads.shape[2])
    weighted_keys = k_heads.astype(jnp.float32) * key_weight[:, :, None]
    own_norm = lax.optimization_barrier(jnp.sum(weighted_keys, axis=0))
    rounded_keys = lax.optimization_barrier(weighted_keys.astype(jnp.bfloat16))
    own_matrix = jnp.einsum('shv,shk->hvk', v_heads.astype(jnp.float32), rounded_keys.astype(jnp.float32))
    return (own_matrix, own_norm, own_max, block_decay)

def readout(intra, carried_state, q_heads, cum_decay):
    intra_num, intra_den, intra_max = intra
    carry_matrix, carry_norm, carry_max, unused_decay = carried_state
    carried_log = cum_decay.T + carry_max[:, None]
    stabilizer = jnp.maximum(intra_max, carried_log)
    intra_scale = jnp.exp(intra_max - stabilizer).T
    carry_scale = jnp.exp(carried_log - stabilizer).T
    q_float = q_heads.astype(jnp.float32)
    carried_num = jnp.einsum('hvk,thk->thv', carry_matrix, q_float, precision=lax.Precision.HIGHEST)
    carried_den = jnp.einsum('hk,thk->th', carry_norm, q_float, precision=lax.Precision.HIGHEST)
    numerator = intra_scale[:, :, None] * intra_num + carry_scale[:, :, None] * carried_num
    denominator = intra_scale * intra_den.T + carry_scale * carried_den
    return (numerator / jnp.maximum(jnp.abs(denominator), 1.0)[:, :, None]).astype(jnp.bfloat16)

def reference(queries, keys, values, forget_gate, input_gate, out_weight):
    block_count = SEQUENCE_TOKENS // TOK_DEV
    group_width = HEAD_TOTAL * DV // N_HEAD
    q_blocks = queries.reshape(block_count, TOK_DEV, HEAD_TOTAL, DQK)
    k_blocks = keys.reshape(block_count, TOK_DEV, HEAD_TOTAL, DQK)
    v_blocks = values.reshape(block_count, TOK_DEV, HEAD_TOTAL, DV)
    f_blocks = forget_gate.reshape(block_count, TOK_DEV, HEAD_TOTAL)
    i_blocks = input_gate.reshape(block_count, TOK_DEV, HEAD_TOTAL)

    def block_step(carried_state, block_inputs):
        q_heads, k_heads, v_heads, forget_block, input_block = block_inputs
        cum_decay = jnp.cumsum(jax.nn.log_sigmoid(forget_block), axis=0)
        intra = intra_terms(q_heads, k_heads, v_heads, cum_decay, input_block)
        own_state = own_terms(k_heads, v_heads, cum_decay, input_block)
        hidden = readout(intra, carried_state, q_heads, cum_decay).reshape(TOK_DEV, HEAD_TOTAL * DV)
        summed = jnp.zeros((TOK_DEV, D), jnp.float32)
        for group_index in range(N_HEAD):
            lower = group_index * group_width
            partial_value = jnp.dot(hidden[:, lower:lower + group_width], out_weight[lower:lower + group_width, :], preferred_element_type=jnp.float32)
            partial_value = lax.optimization_barrier(partial_value.astype(jnp.bfloat16))
            summed = summed + partial_value.astype(jnp.float32)
        return (combine_states(carried_state, own_state), summed.astype(jnp.bfloat16))
    start_state = (jnp.zeros((HEAD_TOTAL, DV, DQK), jnp.float32), jnp.zeros((HEAD_TOTAL, DQK), jnp.float32), jnp.full((HEAD_TOTAL,), -1e+30, jnp.float32), jnp.zeros((HEAD_TOTAL,), jnp.float32))
    unused_state, mixed_blocks = lax.scan(block_step, start_state, (q_blocks, k_blocks, v_blocks, f_blocks, i_blocks))
    mixed = mixed_blocks.reshape(SEQUENCE_TOKENS, D)
    gate_mean = lax.optimization_barrier(jnp.mean(input_gate, axis=0))
    return (mixed, gate_mean)
```

```python
import functools

import jax
import jax.numpy as jnp
from jax import lax
from jax.experimental import pallas as pl
from jax.experimental.pallas import tpu as pltpu
from jax.sharding import PartitionSpec as P

MESH = pl.DeviceIdType.MESH
F32 = jnp.float32
BF16 = jnp.bfloat16
STATE_CHUNKS = 8
ROW_CHUNKS = 4
LOWEST = -1e30


def log_sigmoid(x):
    u = jnp.exp(-jnp.abs(x))
    s = u / (2.0 + u)
    s2 = s * s
    series = jnp.full_like(s, 1.0 / 17.0)
    for odd in (15, 13, 11, 9, 7, 5, 3, 1):
        series = series * s2 + 1.0 / odd
    return jnp.minimum(x, 0.0) - 2.0 * s * series


def kernel(
    n_seq,
    n_head,
    heads,
    dqk,
    dv,
    gates_ref,
    k_ref,
    v_ref,
    q_ref,
    w_hbm,
    out_ref,
    mean_ref,
    w_ref,
    packets,
    maxes,
    norms,
    own,
    x_in,
    fwd,
    y_in,
    carry,
    num,
    stat,
    hid,
    send_a,
    recv_a,
    send_b,
    recv_b,
    acc,
    w_sem,
    p_send,
    p_recv,
    zs_sem,
    zr_sem,
    ys_sem,
    yr_sem,
    as_sem,
    ar_sem,
    bs_sem,
    br_sem,
):
    tokens = q_ref.shape[0]
    cols = out_ref.shape[1]
    groups = n_head // 2
    me = lax.axis_index("seq")
    head = lax.axis_index("head")
    slow, fast = me // 2, lax.rem(me, 2)
    last = n_seq // 2 - 1
    group, core = head // 2, lax.rem(head, 2)

    barrier = pltpu.get_barrier_semaphore()
    for d in range(1, n_seq):
        pl.semaphore_signal(
            barrier, 1, device_id={"seq": lax.rem(me + d, n_seq)}, device_id_type=MESH
        )
    for d in range(1, n_head):
        pl.semaphore_signal(
            barrier, 1, device_id={"head": lax.rem(head + d, n_head)}, device_id_type=MESH
        )
    w_copy = pltpu.make_async_copy(w_hbm, w_ref, w_sem)
    w_copy.start()

    gates = gates_ref[...]
    pad = gates.shape[0]
    row_id = lax.broadcasted_iota(jnp.int32, (tokens, tokens), 0)
    col_id = lax.broadcasted_iota(jnp.int32, (tokens, tokens), 1)
    upper = (row_id <= col_id).astype(F32)
    causal = row_id >= col_id
    cum = jnp.dot(
        log_sigmoid(gates), upper, precision=lax.Precision.HIGHEST, preferred_element_type=F32
    )
    inp = gates[heads : 2 * heads, :]
    cum = cum[:heads, :]
    drive = inp - cum
    decay = cum[:, tokens - 1 : tokens]
    own_log = decay + drive
    own_max = jnp.max(own_log, axis=1, keepdims=True)
    key_weight = jnp.exp(own_log - own_max) * (1.0 / dqk**0.5)
    stacked = jnp.concatenate(
        [cum, key_weight, jnp.zeros((128 - 2 * heads, tokens), F32)], axis=0
    )
    columns = stacked.T

    width = packets.shape[2]
    for h in range(heads):
        kf = k_ref[:, h * dqk : (h + 1) * dqk].astype(F32)
        wk = kf * columns[:, heads + h : heads + h + 1]
        packets[me, h : h + 1, 0:dqk] = jnp.sum(wk, axis=0, keepdims=True)
        packets[me, h : h + 1, dqk:width] = jnp.zeros((1, width - dqk), F32)
        packets[me, heads + h : heads + h + 1, :] = jnp.broadcast_to(
            own_max[h : h + 1, :], (1, width)
        )
        packets[me, 2 * heads + h : 2 * heads + h + 1, :] = jnp.broadcast_to(
            decay[h : h + 1, :], (1, width)
        )
        packets[me, 3 * heads + h : 3 * heads + h + 1, :] = jnp.broadcast_to(
            jnp.sum(inp[h : h + 1, :], axis=1, keepdims=True), (1, width)
        )
        own[h * dqk : (h + 1) * dqk, :] = lax.dot_general(
            wk.astype(BF16),
            v_ref[:, h * dv : (h + 1) * dv],
            (((0,), (0,)), ((), ())),
            preferred_element_type=F32,
        ).astype(BF16)

    chunk = heads * dqk // STATE_CHUNKS

    def part(ref, c):
        return ref.at[pl.ds(c * chunk, chunk)]

    def z_copy(src, c):
        return pltpu.make_async_remote_copy(
            src_ref=part(src, c),
            dst_ref=part(x_in, c),
            send_sem=zs_sem.at[c],
            recv_sem=zr_sem.at[c],
            device_id={"seq": jnp.minimum(me + 2, n_seq - 2 + fast)},
            device_id_type=MESH,
        )

    def y_copy(src, c):
        return pltpu.make_async_remote_copy(
            src_ref=part(src, c),
            dst_ref=part(y_in, c),
            send_sem=ys_sem.at[c],
            recv_sem=yr_sem.at[c],
            device_id={"seq": me + 1 - 2 * fast},
            device_id_type=MESH,
        )

    def p_copy(d):
        return pltpu.make_async_remote_copy(
            src_ref=packets.at[me],
            dst_ref=packets.at[me],
            send_sem=p_send.at[d],
            recv_sem=p_recv.at[d],
            device_id={"seq": lax.rem(me + d, n_seq)},
            device_id_type=MESH,
        )

    pl.semaphore_wait(barrier, n_seq + n_head - 2)
    for d in range(1, n_seq):
        p_copy(d).start()
    first = slow == 0
    feeds = slow < last

    @pl.when(first)
    def _():
        for c in range(STATE_CHUNKS):
            z_copy(own, c).start()

            @pl.when(fast == 0)
            def _():
                y_copy(own, c).start()

    for h in range(heads):
        masked = jnp.where(causal, drive[h : h + 1, :], LOWEST)
        top = jnp.max(masked, axis=1, keepdims=True)
        factors = jnp.exp(masked - top)
        scores = lax.dot_general(
            q_ref[:, h * dqk : (h + 1) * dqk],
            k_ref[:, h * dqk : (h + 1) * dqk],
            (((1,), (1,)), ((), ())),
            preferred_element_type=F32,
        ) * (1.0 / dqk**0.5)
        weighted = factors * scores
        cum_col = columns[:, h : h + 1]
        stat[h] = jnp.concatenate(
            [
                jnp.broadcast_to(jnp.sum(weighted, axis=1, keepdims=True), (tokens, 128)),
                jnp.broadcast_to(top + cum_col, (tokens, 128)),
                jnp.broadcast_to(cum_col, (tokens, 128)),
            ],
            axis=1,
        )
        num[:, h * dv : (h + 1) * dv] = jnp.dot(
            weighted.astype(BF16), v_ref[:, h * dv : (h + 1) * dv], preferred_element_type=F32
        )

    for d in range(1, n_seq):
        pltpu.make_async_remote_copy(
            src_ref=packets.at[me],
            dst_ref=packets.at[lax.rem(me + n_seq - d, n_seq)],
            send_sem=p_send.at[d],
            recv_sem=p_recv.at[d],
            device_id={"seq": lax.rem(me + d, n_seq)},
            device_id_type=MESH,
        ).wait()

    big = jnp.full((heads, width), LOWEST, F32)
    nrm = jnp.zeros((heads, width), F32)
    total = jnp.zeros((heads, width), F32)
    maxes[0] = big
    norms[0] = nrm
    for i in range(n_seq):
        block = packets[i]
        m_i = block[heads : 2 * heads, :]
        g_i = block[2 * heads : 3 * heads, :]
        total = total + block[3 * heads : 4 * heads, :]
        merged = jnp.maximum(big + g_i, m_i)
        nrm = jnp.exp(big + g_i - merged) * nrm + jnp.exp(m_i - merged) * block[0:heads, :]
        big = merged
        maxes[i + 1] = big
        norms[i + 1] = nrm
    mean_ref[...] = total[:, 0:128] * (1.0 / (tokens * n_seq))

    prev = jnp.maximum(me - 1, 0)
    prev2 = jnp.maximum(me - 2, 0)
    max_me = maxes[me]
    max_next = maxes[me + 1]
    m_own = packets[me][heads : 2 * heads, :]
    g_own = packets[me][2 * heads : 3 * heads, :]
    g_prev = packets[prev][2 * heads : 3 * heads, :]
    m_prev = packets[prev][heads : 2 * heads, :]
    m_prev2 = packets[prev2][heads : 2 * heads, :]
    x_ref_max = jnp.where(slow == 1, m_prev2, maxes[prev])
    y_ref_max = jnp.where((slow == 1) & (fast == 0), m_prev, max_me)
    x_next = jnp.exp(jnp.minimum(x_ref_max + g_prev + g_own - max_next, 0.0))
    own_next = jnp.exp(m_own - max_next)
    x_here = jnp.exp(jnp.minimum(x_ref_max + g_prev - max_me, 0.0))
    y_here = jnp.exp(jnp.minimum(y_ref_max - max_me, 0.0))

    def scale(array, c):
        h = c * chunk // dqk
        return array[h : h + 1, :]

    @pl.when(slow > 0)
    def _():
        for c in range(STATE_CHUNKS):
            z_copy(x_in, c).wait_recv()

            @pl.when(fast == 1)
            def _():
                y_copy(x_in, c).start()

            @pl.when(feeds | (fast == 0))
            def _():
                rows = pl.ds(c * chunk, chunk)
                fwd[rows, :] = (
                    x_in[rows, :].astype(F32) * scale(x_next, c)
                    + own[rows, :].astype(F32) * scale(own_next, c)
                ).astype(BF16)

                @pl.when(feeds)
                def _():
                    z_copy(fwd, c).start()

                @pl.when(fast == 0)
                def _():
                    y_copy(fwd, c).start()

    @pl.when(me == 0)
    def _():
        carry[...] = jnp.zeros_like(carry)

    @pl.when(me > 0)
    def _():
        for c in range(STATE_CHUNKS):
            rows = pl.ds(c * chunk, chunk)
            y_copy(y_in, c).wait_recv()
            got = y_in[rows, :].astype(F32) * scale(y_here, c)

            @pl.when(first)
            def _():
                carry[rows, :] = got.astype(BF16)

            @pl.when(slow > 0)
            def _():
                carry[rows, :] = (got + x_in[rows, :].astype(F32) * scale(x_here, c)).astype(BF16)

    w_copy.wait()

    span = tokens // ROW_CHUNKS
    norm_me = norms[me]

    def a_copy(gg, r):
        return pltpu.make_async_remote_copy(
            src_ref=send_a.at[gg, pl.ds(r * span, span)],
            dst_ref=recv_a.at[gg, pl.ds(r * span, span)],
            send_sem=as_sem.at[gg, r],
            recv_sem=ar_sem.at[gg, r],
            device_id={"head": head + 1 - 2 * core},
            device_id_type=MESH,
        )

    def b_copy(gg, r):
        return pltpu.make_async_remote_copy(
            src_ref=send_b.at[gg - 1, pl.ds(r * span, span)],
            dst_ref=recv_b.at[gg - 1, pl.ds(r * span, span)],
            send_sem=bs_sem.at[gg - 1, r],
            recv_sem=br_sem.at[gg - 1, r],
            device_id={"head": lax.rem(group + gg, groups) * 2 + core},
            device_id_type=MESH,
        )

    def project(gg, side, r):
        place = lax.rem(group + gg, groups) * 2 + side
        return jnp.dot(
            hid[pl.ds(pl.multiple_of(r * span, span), span), :],
            w_ref[:, pl.ds(pl.multiple_of(place * cols, cols), cols)],
            preferred_element_type=F32,
        )

    def rows_of(r):
        return pl.ds(pl.multiple_of(r * span, span), span)

    def hidden(r):
        rows = rows_of(r)
        for h in range(heads):
            q = q_ref[rows, h * dqk : (h + 1) * dqk]
            carried_num = jnp.dot(
                q, carry[h * dqk : (h + 1) * dqk, :], preferred_element_type=F32
            )
            carried_den = jnp.sum(q.astype(F32) * norm_me[h : h + 1, 0:dqk], axis=1, keepdims=True)
            stats = stat[h, rows, :]
            intra_den = stats[:, 0:1]
            intra_max = stats[:, 128:129]
            carried_log = stats[:, 256:257] + max_me[h : h + 1, 0:1]
            stabilizer = jnp.maximum(intra_max, carried_log)
            a = jnp.exp(intra_max - stabilizer)
            c = jnp.exp(carried_log - stabilizer)
            den = jnp.maximum(jnp.abs(a * intra_den + c * carried_den), 1.0)
            hid[rows, h * dv : (h + 1) * dv] = (
                num[rows, h * dv : (h + 1) * dv] * (a / den) + carried_num * (c / den)
            ).astype(BF16)

    def sweep(r, _):
        @pl.when(r < ROW_CHUNKS)
        def _():
            hidden(r)
            for gg in range(1, groups):
                send_a[gg, rows_of(r), :] = project(gg, 1 - core, r).astype(BF16)
                a_copy(gg, r).start()

        @pl.when(r > 0)
        def _():
            rr = r - 1
            for gg in range(1, groups):
                mine = project(gg, core, rr)
                a_copy(gg, rr).wait_recv()
                send_b[gg - 1, rows_of(rr), :] = (
                    mine + recv_a[gg, rows_of(rr), :].astype(F32)
                ).astype(BF16)
                b_copy(gg, rr).start()

        return 0

    lax.fori_loop(0, ROW_CHUNKS + 1, sweep, 0)

    def local_a(r, _):
        send_a[0, rows_of(r), :] = project(0, 1 - core, r).astype(BF16)
        a_copy(0, r).start()
        return 0

    lax.fori_loop(0, ROW_CHUNKS, local_a, 0)

    def local_b(r, _):
        mine = project(0, core, r)
        a_copy(0, r).wait_recv()
        acc[rows_of(r), :] = mine + recv_a[0, rows_of(r), :].astype(F32)
        return 0

    lax.fori_loop(0, ROW_CHUNKS, local_b, 0)

    def finish(r, _):
        value = acc[rows_of(r), :]
        for gg in range(1, groups):
            b_copy(gg, r).wait_recv()
            value = value + recv_b[gg - 1, rows_of(r), :].astype(F32)
        out_ref[rows_of(r), :] = value.astype(out_ref.dtype)
        return 0

    lax.fori_loop(0, ROW_CHUNKS, finish, 0)

    for c in range(STATE_CHUNKS):

        @pl.when(feeds)
        def _():
            z_copy(own, c).wait_send()

        @pl.when((fast == 0) | (slow > 0))
        def _():
            y_copy(own, c).wait_send()

    for r in range(ROW_CHUNKS):
        for gg in range(groups):
            a_copy(gg, r).wait_send()
        for gg in range(1, groups):
            b_copy(gg, r).wait_send()


def shards(n_seq, n_head, queries, keys, values, forget_gate, input_gate, out_weight):
    tokens = queries.shape[0]
    heads = forget_gate.shape[1]
    dqk = queries.shape[1] // heads
    dv = values.shape[1] // heads
    cols = out_weight.shape[1] // n_head
    groups = n_head // 2
    pad = -(-2 * heads // 8) * 8
    gates = jnp.concatenate(
        [
            forget_gate.T,
            input_gate.T,
            jnp.zeros((pad - 2 * heads, tokens), F32),
        ],
        axis=0,
    )
    width = max(dqk, dv)
    state = (heads * dqk, dv)
    vmem = pl.BlockSpec(memory_space=pltpu.VMEM)
    dma = pltpu.SemaphoreType.DMA
    mixed, mean = pl.pallas_call(
        functools.partial(kernel, n_seq, n_head, heads, dqk, dv),
        out_shape=(
            jax.ShapeDtypeStruct((tokens, cols), BF16),
            jax.ShapeDtypeStruct((heads, 128), F32),
        ),
        in_specs=[vmem] * 4 + [pl.BlockSpec(memory_space=pl.ANY)],
        out_specs=(vmem, vmem),
        scratch_shapes=[
            pltpu.VMEM(out_weight.shape, BF16),
            pltpu.VMEM((n_seq, 4 * heads, width), F32),
            pltpu.VMEM((n_seq + 1, heads, width), F32),
            pltpu.VMEM((n_seq + 1, heads, width), F32),
            pltpu.VMEM(state, BF16),
            pltpu.VMEM(state, BF16),
            pltpu.VMEM(state, BF16),
            pltpu.VMEM(state, BF16),
            pltpu.VMEM(state, BF16),
            pltpu.VMEM((tokens, heads * dv), F32),
            pltpu.VMEM((heads, tokens, 384), F32),
            pltpu.VMEM((tokens, heads * dv), BF16),
            pltpu.VMEM((groups, tokens, cols), BF16),
            pltpu.VMEM((groups, tokens, cols), BF16),
            pltpu.VMEM((groups - 1, tokens, cols), BF16),
            pltpu.VMEM((groups - 1, tokens, cols), BF16),
            pltpu.VMEM((tokens, cols), F32),
            dma,
            dma((n_seq,)),
            dma((n_seq,)),
            dma((STATE_CHUNKS,)),
            dma((STATE_CHUNKS,)),
            dma((STATE_CHUNKS,)),
            dma((STATE_CHUNKS,)),
            dma((groups, ROW_CHUNKS)),
            dma((groups, ROW_CHUNKS)),
            dma((groups - 1, ROW_CHUNKS)),
            dma((groups - 1, ROW_CHUNKS)),
        ],
        compiler_params=pltpu.CompilerParams(
            collective_id=0, has_side_effects=True, vmem_limit_bytes=60 * 1024 * 1024
        ),
    )(gates, keys, values, queries, out_weight)
    return mixed, mean[:, 0]


def solution(mesh):
    placed = (
        P("seq", "head"),
        P("seq", "head"),
        P("seq", "head"),
        P("seq", "head"),
        P("seq", "head"),
        P("head", None),
    )
    return jax.shard_map(
        functools.partial(shards, mesh.shape["seq"], mesh.shape["head"]),
        mesh=mesh,
        in_specs=placed,
        out_specs=(P("seq", "head"), P("head")),
        check_vma=False,
    )
```

```python
import functools

import jax
import jax.numpy as jnp
from jax import lax
from jax.experimental import pallas as pl
from jax.experimental.pallas import tpu as pltpu
from jax.sharding import PartitionSpec as P

MESH = pl.DeviceIdType.MESH
F32 = jnp.float32
BF16 = jnp.bfloat16
STATE_CHUNKS = 16
ROW_CHUNKS = 4
TAIL_CHUNKS = 2
LOWEST = -1e30


def log_sigmoid(x):
    u = jnp.exp(-jnp.abs(x))
    s = u / (2.0 + u)
    s2 = s * s
    series = jnp.full_like(s, 1.0 / 17.0)
    for odd in (15, 13, 11, 9, 7, 5, 3, 1):
        series = series * s2 + 1.0 / odd
    return jnp.minimum(x, 0.0) - 2.0 * s * series


def kernel(
    n_seq,
    n_head,
    heads,
    dqk,
    dv,
    forget_ref,
    input_ref,
    k_hbm,
    v_hbm,
    q_hbm,
    w_hbm,
    acc_hbm,
    recv_b,
    mean_ref,
    k_ref,
    v_ref,
    q_ref,
    w_ref,
    packets,
    maxes,
    norms,
    wkb,
    own,
    x_in,
    fwd,
    y_in,
    carry,
    num,
    stat,
    hid,
    send_a,
    recv_a,
    send_b,
    acc,
    in_sem,
    w_sem,
    p_send,
    p_recv,
    zs_sem,
    zr_sem,
    ys_sem,
    yr_sem,
    as_sem,
    ar_sem,
    bs_sem,
    br_sem,
    acc_sem,
):
    loads = [
        pltpu.make_async_copy(src, dst, in_sem.at[i])
        for i, (src, dst) in enumerate(((k_hbm, k_ref), (v_hbm, v_ref), (q_hbm, q_ref)))
    ]
    for load in loads:
        load.start()
    tokens = q_ref.shape[0]
    cols = acc_hbm.shape[1]
    groups = n_head // 2
    me = lax.axis_index("seq")
    head = lax.axis_index("head")
    slow, fast = me // 2, lax.rem(me, 2)
    last = n_seq // 2 - 1
    group, core = head // 2, lax.rem(head, 2)

    barrier = pltpu.get_barrier_semaphore()
    for d in range(1, n_seq):
        pl.semaphore_signal(
            barrier, 1, device_id={"seq": lax.rem(me + d, n_seq)}, device_id_type=MESH
        )
    for d in range(1, n_head):
        pl.semaphore_signal(
            barrier, 1, device_id={"head": lax.rem(head + d, n_head)}, device_id_type=MESH
        )
    w_copy = pltpu.make_async_copy(w_hbm, w_ref, w_sem)
    w_copy.start()

    row_id = lax.broadcasted_iota(jnp.int32, (tokens, tokens), 0)
    col_id = lax.broadcasted_iota(jnp.int32, (tokens, tokens), 1)
    upper = (row_id <= col_id).astype(F32).astype(BF16)
    causal = row_id >= col_id
    inp = input_ref[...]
    log_forget = jnp.concatenate(
        [log_sigmoid(forget_ref[...]), jnp.zeros((8 - heads % 8, tokens), F32)], axis=0
    )
    high = log_forget.astype(BF16).astype(F32)
    middle = (log_forget - high).astype(BF16).astype(F32)
    pieces = jnp.concatenate([high, middle, log_forget - high - middle], axis=0)
    sums = jnp.dot(pieces.astype(BF16), upper, preferred_element_type=F32)
    pad = log_forget.shape[0]
    cum = (sums[2 * pad :] + sums[pad : 2 * pad] + sums[:pad])[:heads, :]
    drive = inp - cum
    decay = cum[:, tokens - 1 : tokens]
    own_log = decay + drive
    own_max = jnp.max(own_log, axis=1, keepdims=True)
    key_weight = jnp.exp(own_log - own_max) * (1.0 / dqk**0.5)
    stacked = jnp.concatenate(
        [cum, key_weight, jnp.zeros((128 - 2 * heads, tokens), F32)], axis=0
    )
    columns = stacked.T

    width = packets.shape[2]
    loads[0].wait()
    for h in range(heads):
        kf = k_ref[:, h * dqk : (h + 1) * dqk].astype(F32)
        wk = kf * columns[:, heads + h : heads + h + 1]
        packets[me, h : h + 1, 0:dqk] = jnp.sum(wk, axis=0, keepdims=True)
        packets[me, h : h + 1, dqk:width] = jnp.zeros((1, width - dqk), F32)
        packets[me, heads + h : heads + h + 1, :] = jnp.broadcast_to(
            own_max[h : h + 1, :], (1, width)
        )
        packets[me, 2 * heads + h : 2 * heads + h + 1, :] = jnp.broadcast_to(
            decay[h : h + 1, :], (1, width)
        )
        packets[me, 3 * heads + h : 3 * heads + h + 1, :] = jnp.broadcast_to(
            jnp.sum(inp[h : h + 1, :], axis=1, keepdims=True), (1, width)
        )
        wkb[:, h * dqk : (h + 1) * dqk] = wk.astype(BF16)

    chunk = heads * dqk // STATE_CHUNKS

    def part(ref, c):
        return ref.at[pl.ds(c * chunk, chunk)]

    def z_copy(src, c):
        return pltpu.make_async_remote_copy(
            src_ref=part(src, c),
            dst_ref=part(x_in, c),
            send_sem=zs_sem.at[c],
            recv_sem=zr_sem.at[c],
            device_id={"seq": jnp.minimum(me + 2, n_seq - 2 + fast)},
            device_id_type=MESH,
        )

    def y_copy(src, c):
        return pltpu.make_async_remote_copy(
            src_ref=part(src, c),
            dst_ref=part(y_in, c),
            send_sem=ys_sem.at[c],
            recv_sem=yr_sem.at[c],
            device_id={"seq": me + 1 - 2 * fast},
            device_id_type=MESH,
        )

    def p_copy(d):
        return pltpu.make_async_remote_copy(
            src_ref=packets.at[me],
            dst_ref=packets.at[me],
            send_sem=p_send.at[d],
            recv_sem=p_recv.at[d],
            device_id={"seq": lax.rem(me + d, n_seq)},
            device_id_type=MESH,
        )

    pl.semaphore_wait(barrier, n_seq + n_head - 2)
    for d in range(1, n_seq):
        p_copy(d).start()
    first = slow == 0
    feeds = slow < last

    loads[1].wait()
    per_head = STATE_CHUNKS // heads
    for h in range(heads):
        own[h * dqk : (h + 1) * dqk, :] = lax.dot_general(
            wkb[:, h * dqk : (h + 1) * dqk],
            v_ref[:, h * dv : (h + 1) * dv],
            (((0,), (0,)), ((), ())),
            preferred_element_type=F32,
        ).astype(BF16)

        @pl.when(first)
        def _():
            for c in range(h * per_head, (h + 1) * per_head):
                z_copy(own, c).start()

                @pl.when(fast == 0)
                def _():
                    y_copy(own, c).start()

    loads[2].wait()
    for h in range(heads):
        masked = jnp.where(causal, drive[h : h + 1, :], LOWEST)
        top = jnp.max(masked, axis=1, keepdims=True)
        factors = jnp.exp(masked - top)
        scores = lax.dot_general(
            q_ref[:, h * dqk : (h + 1) * dqk],
            k_ref[:, h * dqk : (h + 1) * dqk],
            (((1,), (1,)), ((), ())),
            preferred_element_type=F32,
        ) * (1.0 / dqk**0.5)
        weighted = factors * scores
        cum_col = columns[:, h : h + 1]
        stat[h] = jnp.concatenate(
            [
                jnp.broadcast_to(jnp.sum(weighted, axis=1, keepdims=True), (tokens, 128)),
                jnp.broadcast_to(top + cum_col, (tokens, 128)),
                jnp.broadcast_to(cum_col, (tokens, 128)),
            ],
            axis=1,
        )
        num[:, h * dv : (h + 1) * dv] = jnp.dot(
            weighted.astype(BF16), v_ref[:, h * dv : (h + 1) * dv], preferred_element_type=F32
        )

    for d in range(1, n_seq):
        pltpu.make_async_remote_copy(
            src_ref=packets.at[me],
            dst_ref=packets.at[lax.rem(me + n_seq - d, n_seq)],
            send_sem=p_send.at[d],
            recv_sem=p_recv.at[d],
            device_id={"seq": lax.rem(me + d, n_seq)},
            device_id_type=MESH,
        ).wait()

    big = jnp.full((heads, width), LOWEST, F32)
    nrm = jnp.zeros((heads, width), F32)
    total = jnp.zeros((heads, width), F32)
    maxes[0] = big
    norms[0] = nrm
    for i in range(n_seq):
        block = packets[i]
        m_i = block[heads : 2 * heads, :]
        g_i = block[2 * heads : 3 * heads, :]
        total = total + block[3 * heads : 4 * heads, :]
        merged = jnp.maximum(big + g_i, m_i)
        nrm = jnp.exp(big + g_i - merged) * nrm + jnp.exp(m_i - merged) * block[0:heads, :]
        big = merged
        maxes[i + 1] = big
        norms[i + 1] = nrm
    for h in range(heads):
        mean_ref[h] = total[h, 0] * (1.0 / (tokens * n_seq))

    prev = jnp.maximum(me - 1, 0)
    prev2 = jnp.maximum(me - 2, 0)
    max_me = maxes[me]
    max_next = maxes[me + 1]
    m_own = packets[me][heads : 2 * heads, :]
    g_own = packets[me][2 * heads : 3 * heads, :]
    g_prev = packets[prev][2 * heads : 3 * heads, :]
    m_prev = packets[prev][heads : 2 * heads, :]
    m_prev2 = packets[prev2][heads : 2 * heads, :]
    x_ref_max = jnp.where(slow == 1, m_prev2, maxes[prev])
    y_ref_max = jnp.where((slow == 1) & (fast == 0), m_prev, max_me)
    x_next = jnp.exp(jnp.minimum(x_ref_max + g_prev + g_own - max_next, 0.0))
    own_next = jnp.exp(m_own - max_next)
    x_here = jnp.exp(jnp.minimum(x_ref_max + g_prev - max_me, 0.0))
    y_here = jnp.exp(jnp.minimum(y_ref_max - max_me, 0.0))

    def scale(array, c):
        h = c * chunk // dqk
        return array[h : h + 1, :]

    @pl.when(slow > 0)
    def _():
        for c in range(STATE_CHUNKS):
            z_copy(x_in, c).wait_recv()

            @pl.when(fast == 1)
            def _():
                y_copy(x_in, c).start()

            @pl.when(feeds | (fast == 0))
            def _():
                rows = pl.ds(c * chunk, chunk)
                fwd[rows, :] = (
                    x_in[rows, :].astype(F32) * scale(x_next, c)
                    + own[rows, :].astype(F32) * scale(own_next, c)
                ).astype(BF16)

                @pl.when(feeds)
                def _():
                    z_copy(fwd, c).start()

                @pl.when(fast == 0)
                def _():
                    y_copy(fwd, c).start()

    @pl.when(me == 0)
    def _():
        carry[...] = jnp.zeros_like(carry)

    @pl.when(me > 0)
    def _():
        for c in range(STATE_CHUNKS):
            rows = pl.ds(c * chunk, chunk)
            y_copy(y_in, c).wait_recv()
            got = y_in[rows, :].astype(F32) * scale(y_here, c)

            @pl.when(first)
            def _():
                carry[rows, :] = got.astype(BF16)

            @pl.when(slow > 0)
            def _():
                carry[rows, :] = (got + x_in[rows, :].astype(F32) * scale(x_here, c)).astype(BF16)

    w_copy.wait()

    span = tokens // ROW_CHUNKS
    norm_me = norms[me]

    def a_copy(gg, r):
        return pltpu.make_async_remote_copy(
            src_ref=send_a.at[gg, pl.ds(r * span, span)],
            dst_ref=recv_a.at[gg, pl.ds(r * span, span)],
            send_sem=as_sem.at[gg, r],
            recv_sem=ar_sem.at[gg, r],
            device_id={"head": head + 1 - 2 * core},
            device_id_type=MESH,
        )

    def b_copy(gg, r):
        return pltpu.make_async_remote_copy(
            src_ref=send_b.at[gg - 1, pl.ds(r * span, span)],
            dst_ref=recv_b.at[gg - 1, pl.ds(r * span, span)],
            send_sem=bs_sem.at[gg - 1, r],
            recv_sem=br_sem.at[gg - 1, r],
            device_id={"head": lax.rem(group + gg, groups) * 2 + core},
            device_id_type=MESH,
        )

    def project(gg, side, r):
        place = lax.rem(group + gg, groups) * 2 + side
        return jnp.dot(
            hid[pl.ds(pl.multiple_of(r * span, span), span), :],
            w_ref[:, pl.ds(pl.multiple_of(place * cols, cols), cols)],
            preferred_element_type=F32,
        )

    def rows_of(r):
        return pl.ds(pl.multiple_of(r * span, span), span)

    def hidden(r):
        rows = rows_of(r)
        for h in range(heads):
            q = q_ref[rows, h * dqk : (h + 1) * dqk]
            carried_num = jnp.dot(
                q, carry[h * dqk : (h + 1) * dqk, :], preferred_element_type=F32
            )
            carried_den = jnp.sum(q.astype(F32) * norm_me[h : h + 1, 0:dqk], axis=1, keepdims=True)
            stats = stat[h, rows, :]
            intra_den = stats[:, 0:1]
            intra_max = stats[:, 128:129]
            carried_log = stats[:, 256:257] + max_me[h : h + 1, 0:1]
            stabilizer = jnp.maximum(intra_max, carried_log)
            a = jnp.exp(intra_max - stabilizer)
            c = jnp.exp(carried_log - stabilizer)
            den = jnp.maximum(jnp.abs(a * intra_den + c * carried_den), 1.0)
            hid[rows, h * dv : (h + 1) * dv] = (
                num[rows, h * dv : (h + 1) * dv] * (a / den) + carried_num * (c / den)
            ).astype(BF16)

    def sweep(r, _):
        @pl.when(r < ROW_CHUNKS)
        def _():
            hidden(r)
            for gg in range(1, groups):
                send_a[gg, rows_of(r), :] = project(gg, 1 - core, r).astype(BF16)
                a_copy(gg, r).start()

        @pl.when(r > 0)
        def _():
            rr = r - 1
            for gg in range(1, groups):
                mine = project(gg, core, rr)
                a_copy(gg, rr).wait_recv()
                send_b[gg - 1, rows_of(rr), :] = (
                    mine + recv_a[gg, rows_of(rr), :].astype(F32)
                ).astype(BF16)
                b_copy(gg, rr).start()

        return 0

    lax.fori_loop(0, ROW_CHUNKS + 1, sweep, 0)

    def local_a(r, _):
        send_a[0, rows_of(r), :] = project(0, 1 - core, r).astype(BF16)
        a_copy(0, r).start()
        return 0

    lax.fori_loop(0, ROW_CHUNKS, local_a, 0)

    def acc_copy(r):
        return pltpu.make_async_copy(acc.at[rows_of(r)], acc_hbm.at[rows_of(r)], acc_sem.at[r])

    def local_b(r, _):
        mine = project(0, core, r)
        a_copy(0, r).wait_recv()
        acc[rows_of(r), :] = (mine + recv_a[0, rows_of(r), :].astype(F32)).astype(BF16)
        acc_copy(r).start()
        return 0

    lax.fori_loop(0, ROW_CHUNKS, local_b, 0)

    for c in range(STATE_CHUNKS):

        @pl.when(feeds)
        def _():
            z_copy(own, c).wait_send()

        @pl.when((fast == 0) | (slow > 0))
        def _():
            y_copy(own, c).wait_send()

    for r in range(ROW_CHUNKS):
        acc_copy(r).wait()
        for gg in range(groups):
            a_copy(gg, r).wait_send()
        for gg in range(1, groups):
            b_copy(gg, r).wait_send()
            b_copy(gg, r).wait_recv()


def finish(acc_ref, recv_ref, mean_ref, out_ref, final_ref):
    value = acc_ref[...].astype(F32)
    for gg in range(recv_ref.shape[0]):
        value = value + recv_ref[gg].astype(F32)
    out_ref[...] = value.astype(out_ref.dtype)
    for h in range(final_ref.shape[0]):
        final_ref[h] = mean_ref[h]


def shards(n_seq, n_head, queries, keys, values, forget_gate, input_gate, out_weight):
    tokens = queries.shape[0]
    heads = forget_gate.shape[1]
    dqk = queries.shape[1] // heads
    dv = values.shape[1] // heads
    cols = out_weight.shape[1] // n_head
    groups = n_head // 2
    width = max(dqk, dv)
    state = (heads * dqk, dv)
    vmem = pl.BlockSpec(memory_space=pltpu.VMEM)
    dma = pltpu.SemaphoreType.DMA
    hbm = pl.BlockSpec(memory_space=pltpu.HBM)
    smem = pl.BlockSpec(memory_space=pltpu.SMEM)
    kept, received, mean = pl.pallas_call(
        functools.partial(kernel, n_seq, n_head, heads, dqk, dv),
        out_shape=(
            jax.ShapeDtypeStruct((tokens, cols), BF16),
            jax.ShapeDtypeStruct((groups - 1, tokens, cols), BF16),
            jax.ShapeDtypeStruct((heads,), F32),
        ),
        in_specs=[vmem] * 2 + [hbm] * 4,
        out_specs=(hbm, hbm, smem),
        scratch_shapes=[
            pltpu.VMEM(keys.shape, BF16),
            pltpu.VMEM(values.shape, BF16),
            pltpu.VMEM(queries.shape, BF16),
            pltpu.VMEM(out_weight.shape, BF16),
            pltpu.VMEM((n_seq, 4 * heads, width), F32),
            pltpu.VMEM((n_seq + 1, heads, width), F32),
            pltpu.VMEM((n_seq + 1, heads, width), F32),
            pltpu.VMEM((tokens, heads * dqk), BF16),
            pltpu.VMEM(state, BF16),
            pltpu.VMEM(state, BF16),
            pltpu.VMEM(state, BF16),
            pltpu.VMEM(state, BF16),
            pltpu.VMEM(state, BF16),
            pltpu.VMEM((tokens, heads * dv), F32),
            pltpu.VMEM((heads, tokens, 384), F32),
            pltpu.VMEM((tokens, heads * dv), BF16),
            pltpu.VMEM((groups, tokens, cols), BF16),
            pltpu.VMEM((groups, tokens, cols), BF16),
            pltpu.VMEM((groups - 1, tokens, cols), BF16),
            pltpu.VMEM((tokens, cols), BF16),
            dma((3,)),
            dma,
            dma((n_seq,)),
            dma((n_seq,)),
            dma((STATE_CHUNKS,)),
            dma((STATE_CHUNKS,)),
            dma((STATE_CHUNKS,)),
            dma((STATE_CHUNKS,)),
            dma((groups, ROW_CHUNKS)),
            dma((groups, ROW_CHUNKS)),
            dma((groups - 1, ROW_CHUNKS)),
            dma((groups - 1, ROW_CHUNKS)),
            dma((ROW_CHUNKS,)),
        ],
        compiler_params=pltpu.CompilerParams(
            collective_id=0, has_side_effects=True, vmem_limit_bytes=62 * 1024 * 1024
        ),
    )(forget_gate.T, input_gate.T, keys, values, queries, out_weight)
    span = tokens // TAIL_CHUNKS
    mixed, mean = pl.pallas_call(
        finish,
        grid=(TAIL_CHUNKS,),
        out_shape=(
            jax.ShapeDtypeStruct((tokens, cols), BF16),
            jax.ShapeDtypeStruct((heads,), F32),
        ),
        in_specs=[
            pl.BlockSpec((span, cols), lambda i: (i, 0)),
            pl.BlockSpec((groups - 1, span, cols), lambda i: (0, i, 0)),
            smem,
        ],
        out_specs=(pl.BlockSpec((span, cols), lambda i: (i, 0)), smem),
        compiler_params=pltpu.CompilerParams(vmem_limit_bytes=62 * 1024 * 1024),
    )(kept, received, mean)
    return mixed, mean


def solution(mesh):
    placed = (
        P("seq", "head"),
        P("seq", "head"),
        P("seq", "head"),
        P("seq", "head"),
        P("seq", "head"),
        P("head", None),
    )
    return jax.shard_map(
        functools.partial(shards, mesh.shape["seq"], mesh.shape["head"]),
        mesh=mesh,
        in_specs=placed,
        out_specs=(P("seq", "head"), P("head")),
        check_vma=False,
    )
```

```python
import functools

import jax
import jax.numpy as jnp
from jax import lax
from jax.experimental import pallas as pl
from jax.experimental.pallas import tpu as pltpu
from jax.sharding import PartitionSpec as P

MESH = pl.DeviceIdType.MESH
F32 = jnp.float32
BF16 = jnp.bfloat16
STATE_CHUNKS = 16
ROW_CHUNKS = 4
TAIL_CHUNKS = 2
LOWEST = -1e30


def log_sigmoid(x):
    u = jnp.exp(-jnp.abs(x))
    s = u / (2.0 + u)
    s2 = s * s
    series = jnp.full_like(s, 1.0 / 17.0)
    for odd in (15, 13, 11, 9, 7, 5, 3, 1):
        series = series * s2 + 1.0 / odd
    return jnp.minimum(x, 0.0) - 2.0 * s * series


def kernel(
    n_seq,
    n_head,
    heads,
    dqk,
    dv,
    forget_ref,
    input_ref,
    k_hbm,
    v_hbm,
    q_hbm,
    w_hbm,
    acc_hbm,
    recv_b,
    mean_ref,
    k_ref,
    v_ref,
    q_ref,
    w_ref,
    packets,
    maxes,
    norms,
    wkb,
    own,
    x_in,
    fwd,
    y_in,
    carry,
    num,
    stat,
    hid,
    send_a,
    recv_a,
    send_b,
    acc,
    in_sem,
    w_sem,
    p_send,
    p_recv,
    zs_sem,
    zr_sem,
    ys_sem,
    yr_sem,
    as_sem,
    ar_sem,
    bs_sem,
    br_sem,
    acc_sem,
):
    loads = [
        pltpu.make_async_copy(src, dst, in_sem.at[i])
        for i, (src, dst) in enumerate(((k_hbm, k_ref), (v_hbm, v_ref), (q_hbm, q_ref)))
    ]
    for load in loads:
        load.start()
    tokens = q_ref.shape[0]
    cols = acc_hbm.shape[1]
    groups = n_head // 2
    me = lax.axis_index("seq")
    head = lax.axis_index("head")
    slow, fast = me // 2, lax.rem(me, 2)
    last = n_seq // 2 - 1
    group, core = head // 2, lax.rem(head, 2)

    barrier = pltpu.get_barrier_semaphore()
    for d in range(1, n_seq):
        pl.semaphore_signal(
            barrier, 1, device_id={"seq": lax.rem(me + d, n_seq)}, device_id_type=MESH
        )
    for d in range(1, n_head):
        pl.semaphore_signal(
            barrier, 1, device_id={"head": lax.rem(head + d, n_head)}, device_id_type=MESH
        )
    w_copy = pltpu.make_async_copy(w_hbm, w_ref, w_sem)

    row_id = lax.broadcasted_iota(jnp.int32, (tokens, tokens), 0)
    col_id = lax.broadcasted_iota(jnp.int32, (tokens, tokens), 1)
    upper = (row_id <= col_id).astype(F32).astype(BF16)
    causal = row_id >= col_id
    inp = input_ref[...]
    log_forget = jnp.concatenate(
        [log_sigmoid(forget_ref[...]), jnp.zeros((8 - heads % 8, tokens), F32)], axis=0
    )
    high = log_forget.astype(BF16).astype(F32)
    middle = (log_forget - high).astype(BF16).astype(F32)
    pieces = jnp.concatenate([high, middle, log_forget - high - middle], axis=0)
    sums = jnp.dot(pieces.astype(BF16), upper, preferred_element_type=F32)
    pad = log_forget.shape[0]
    cum = (sums[2 * pad :] + sums[pad : 2 * pad] + sums[:pad])[:heads, :]
    drive = inp - cum
    decay = cum[:, tokens - 1 : tokens]
    own_log = decay + drive
    own_max = jnp.max(own_log, axis=1, keepdims=True)
    key_weight = jnp.exp(own_log - own_max) * (1.0 / dqk**0.5)
    stacked = jnp.concatenate(
        [cum, key_weight, jnp.zeros((128 - 2 * heads, tokens), F32)], axis=0
    )
    columns = stacked.T

    width = packets.shape[2]
    loads[0].wait()
    for h in range(heads):
        kf = k_ref[:, h * dqk : (h + 1) * dqk].astype(F32)
        wk = kf * columns[:, heads + h : heads + h + 1]
        packets[me, h : h + 1, 0:dqk] = jnp.sum(wk, axis=0, keepdims=True)
        packets[me, h : h + 1, dqk:width] = jnp.zeros((1, width - dqk), F32)
        packets[me, heads + h : heads + h + 1, :] = jnp.broadcast_to(
            own_max[h : h + 1, :], (1, width)
        )
        packets[me, 2 * heads + h : 2 * heads + h + 1, :] = jnp.broadcast_to(
            decay[h : h + 1, :], (1, width)
        )
        packets[me, 3 * heads + h : 3 * heads + h + 1, :] = jnp.broadcast_to(
            jnp.sum(inp[h : h + 1, :], axis=1, keepdims=True), (1, width)
        )
        wkb[:, h * dqk : (h + 1) * dqk] = wk.astype(BF16)

    chunk = heads * dqk // STATE_CHUNKS

    def part(ref, c):
        return ref.at[pl.ds(c * chunk, chunk)]

    def z_copy(src, c):
        return pltpu.make_async_remote_copy(
            src_ref=part(src, c),
            dst_ref=part(x_in, c),
            send_sem=zs_sem.at[c],
            recv_sem=zr_sem.at[c],
            device_id={"seq": jnp.minimum(me + 2, n_seq - 2 + fast)},
            device_id_type=MESH,
        )

    def y_copy(src, c):
        return pltpu.make_async_remote_copy(
            src_ref=part(src, c),
            dst_ref=part(y_in, c),
            send_sem=ys_sem.at[c],
            recv_sem=yr_sem.at[c],
            device_id={"seq": me + 1 - 2 * fast},
            device_id_type=MESH,
        )

    def p_copy(d):
        return pltpu.make_async_remote_copy(
            src_ref=packets.at[me],
            dst_ref=packets.at[me],
            send_sem=p_send.at[d],
            recv_sem=p_recv.at[d],
            device_id={"seq": lax.rem(me + d, n_seq)},
            device_id_type=MESH,
        )

    pl.semaphore_wait(barrier, n_seq + n_head - 2)
    for d in range(1, n_seq):
        p_copy(d).start()
    first = slow == 0
    feeds = slow < last

    loads[1].wait()
    w_copy.start()
    per_head = STATE_CHUNKS // heads
    for h in range(heads):
        own[h * dqk : (h + 1) * dqk, :] = lax.dot_general(
            wkb[:, h * dqk : (h + 1) * dqk],
            v_ref[:, h * dv : (h + 1) * dv],
            (((0,), (0,)), ((), ())),
            preferred_element_type=F32,
        ).astype(BF16)

        @pl.when(first)
        def _():
            for c in range(h * per_head, (h + 1) * per_head):
                z_copy(own, c).start()

                @pl.when(fast == 0)
                def _():
                    y_copy(own, c).start()

    loads[2].wait()
    for h in range(heads):
        masked = jnp.where(causal, drive[h : h + 1, :], LOWEST)
        top = jnp.max(masked, axis=1, keepdims=True)
        factors = jnp.exp(masked - top)
        scores = lax.dot_general(
            q_ref[:, h * dqk : (h + 1) * dqk],
            k_ref[:, h * dqk : (h + 1) * dqk],
            (((1,), (1,)), ((), ())),
            preferred_element_type=F32,
        ) * (1.0 / dqk**0.5)
        weighted = factors * scores
        cum_col = columns[:, h : h + 1]
        stat[h] = jnp.concatenate(
            [
                jnp.broadcast_to(jnp.sum(weighted, axis=1, keepdims=True), (tokens, 128)),
                jnp.broadcast_to(top + cum_col, (tokens, 128)),
                jnp.broadcast_to(cum_col, (tokens, 128)),
            ],
            axis=1,
        )
        num[:, h * dv : (h + 1) * dv] = jnp.dot(
            weighted.astype(BF16), v_ref[:, h * dv : (h + 1) * dv], preferred_element_type=F32
        )

    for d in range(1, n_seq):
        pltpu.make_async_remote_copy(
            src_ref=packets.at[me],
            dst_ref=packets.at[lax.rem(me + n_seq - d, n_seq)],
            send_sem=p_send.at[d],
            recv_sem=p_recv.at[d],
            device_id={"seq": lax.rem(me + d, n_seq)},
            device_id_type=MESH,
        ).wait()

    big = jnp.full((heads, width), LOWEST, F32)
    nrm = jnp.zeros((heads, width), F32)
    total = jnp.zeros((heads, width), F32)
    maxes[0] = big
    norms[0] = nrm
    for i in range(n_seq):
        block = packets[i]
        m_i = block[heads : 2 * heads, :]
        g_i = block[2 * heads : 3 * heads, :]
        total = total + block[3 * heads : 4 * heads, :]
        merged = jnp.maximum(big + g_i, m_i)
        nrm = jnp.exp(big + g_i - merged) * nrm + jnp.exp(m_i - merged) * block[0:heads, :]
        big = merged
        maxes[i + 1] = big
        norms[i + 1] = nrm
    for h in range(heads):
        mean_ref[h] = total[h, 0] * (1.0 / (tokens * n_seq))

    prev = jnp.maximum(me - 1, 0)
    prev2 = jnp.maximum(me - 2, 0)
    max_me = maxes[me]
    max_next = maxes[me + 1]
    m_own = packets[me][heads : 2 * heads, :]
    g_own = packets[me][2 * heads : 3 * heads, :]
    g_prev = packets[prev][2 * heads : 3 * heads, :]
    m_prev = packets[prev][heads : 2 * heads, :]
    m_prev2 = packets[prev2][heads : 2 * heads, :]
    x_ref_max = jnp.where(slow == 1, m_prev2, maxes[prev])
    y_ref_max = jnp.where((slow == 1) & (fast == 0), m_prev, max_me)
    x_next = jnp.exp(jnp.minimum(x_ref_max + g_prev + g_own - max_next, 0.0))
    own_next = jnp.exp(m_own - max_next)
    x_here = jnp.exp(jnp.minimum(x_ref_max + g_prev - max_me, 0.0))
    y_here = jnp.exp(jnp.minimum(y_ref_max - max_me, 0.0))

    def scale(array, c):
        h = c * chunk // dqk
        return array[h : h + 1, :]

    @pl.when(slow > 0)
    def _():
        for c in range(STATE_CHUNKS):
            z_copy(x_in, c).wait_recv()

            @pl.when(fast == 1)
            def _():
                y_copy(x_in, c).start()

            @pl.when(feeds | (fast == 0))
            def _():
                rows = pl.ds(c * chunk, chunk)
                fwd[rows, :] = (
                    x_in[rows, :].astype(F32) * scale(x_next, c)
                    + own[rows, :].astype(F32) * scale(own_next, c)
                ).astype(BF16)

                @pl.when(feeds)
                def _():
                    z_copy(fwd, c).start()

                @pl.when(fast == 0)
                def _():
                    y_copy(fwd, c).start()

    @pl.when(me == 0)
    def _():
        carry[...] = jnp.zeros_like(carry)

    @pl.when(me > 0)
    def _():
        for c in range(STATE_CHUNKS):
            rows = pl.ds(c * chunk, chunk)
            y_copy(y_in, c).wait_recv()
            got = y_in[rows, :].astype(F32) * scale(y_here, c)

            @pl.when(first)
            def _():
                carry[rows, :] = got.astype(BF16)

            @pl.when(slow > 0)
            def _():
                carry[rows, :] = (got + x_in[rows, :].astype(F32) * scale(x_here, c)).astype(BF16)

    w_copy.wait()

    span = tokens // ROW_CHUNKS
    norm_me = norms[me]

    def a_copy(gg, r):
        return pltpu.make_async_remote_copy(
            src_ref=send_a.at[gg, pl.ds(r * span, span)],
            dst_ref=recv_a.at[gg, pl.ds(r * span, span)],
            send_sem=as_sem.at[gg, r],
            recv_sem=ar_sem.at[gg, r],
            device_id={"head": head + 1 - 2 * core},
            device_id_type=MESH,
        )

    def b_copy(gg, r):
        return pltpu.make_async_remote_copy(
            src_ref=send_b.at[gg - 1, pl.ds(r * span, span)],
            dst_ref=recv_b.at[gg - 1, pl.ds(r * span, span)],
            send_sem=bs_sem.at[gg - 1, r],
            recv_sem=br_sem.at[gg - 1, r],
            device_id={"head": lax.rem(group + gg, groups) * 2 + core},
            device_id_type=MESH,
        )

    def project(gg, side, r):
        place = lax.rem(group + gg, groups) * 2 + side
        return jnp.dot(
            hid[pl.ds(pl.multiple_of(r * span, span), span), :],
            w_ref[:, pl.ds(pl.multiple_of(place * cols, cols), cols)],
            preferred_element_type=F32,
        )

    def rows_of(r):
        return pl.ds(pl.multiple_of(r * span, span), span)

    def hidden(r):
        rows = rows_of(r)
        for h in range(heads):
            q = q_ref[rows, h * dqk : (h + 1) * dqk]
            carried_num = jnp.dot(
                q, carry[h * dqk : (h + 1) * dqk, :], preferred_element_type=F32
            )
            carried_den = jnp.sum(q.astype(F32) * norm_me[h : h + 1, 0:dqk], axis=1, keepdims=True)
            stats = stat[h, rows, :]
            intra_den = stats[:, 0:1]
            intra_max = stats[:, 128:129]
            carried_log = stats[:, 256:257] + max_me[h : h + 1, 0:1]
            stabilizer = jnp.maximum(intra_max, carried_log)
            a = jnp.exp(intra_max - stabilizer)
            c = jnp.exp(carried_log - stabilizer)
            den = jnp.maximum(jnp.abs(a * intra_den + c * carried_den), 1.0)
            hid[rows, h * dv : (h + 1) * dv] = (
                num[rows, h * dv : (h + 1) * dv] * (a / den) + carried_num * (c / den)
            ).astype(BF16)

    def sweep(r, _):
        @pl.when(r < ROW_CHUNKS)
        def _():
            hidden(r)
            for gg in range(1, groups):
                send_a[gg, rows_of(r), :] = project(gg, 1 - core, r).astype(BF16)
                a_copy(gg, r).start()

        @pl.when(r > 0)
        def _():
            rr = r - 1
            for gg in range(1, groups):
                mine = project(gg, core, rr)
                a_copy(gg, rr).wait_recv()
                send_b[gg - 1, rows_of(rr), :] = (
                    mine + recv_a[gg, rows_of(rr), :].astype(F32)
                ).astype(BF16)
                b_copy(gg, rr).start()

        return 0

    lax.fori_loop(0, ROW_CHUNKS + 1, sweep, 0)

    def local_a(r, _):
        send_a[0, rows_of(r), :] = project(0, 1 - core, r).astype(BF16)
        a_copy(0, r).start()
        return 0

    lax.fori_loop(0, ROW_CHUNKS, local_a, 0)

    def acc_copy(r):
        return pltpu.make_async_copy(acc.at[rows_of(r)], acc_hbm.at[rows_of(r)], acc_sem.at[r])

    def local_b(r, _):
        mine = project(0, core, r)
        a_copy(0, r).wait_recv()
        acc[rows_of(r), :] = (mine + recv_a[0, rows_of(r), :].astype(F32)).astype(BF16)
        acc_copy(r).start()
        return 0

    lax.fori_loop(0, ROW_CHUNKS, local_b, 0)

    for c in range(STATE_CHUNKS):

        @pl.when(feeds)
        def _():
            z_copy(own, c).wait_send()

        @pl.when((fast == 0) | (slow > 0))
        def _():
            y_copy(own, c).wait_send()

    for r in range(ROW_CHUNKS):
        acc_copy(r).wait()
        for gg in range(groups):
            a_copy(gg, r).wait_send()
        for gg in range(1, groups):
            b_copy(gg, r).wait_send()
            b_copy(gg, r).wait_recv()


def finish(acc_ref, recv_ref, mean_ref, out_ref, final_ref):
    value = acc_ref[...].astype(F32)
    for gg in range(recv_ref.shape[0]):
        value = value + recv_ref[gg].astype(F32)
    out_ref[...] = value.astype(out_ref.dtype)
    for h in range(final_ref.shape[0]):
        final_ref[h] = mean_ref[h]


def shards(n_seq, n_head, queries, keys, values, forget_gate, input_gate, out_weight):
    tokens = queries.shape[0]
    heads = forget_gate.shape[1]
    dqk = queries.shape[1] // heads
    dv = values.shape[1] // heads
    cols = out_weight.shape[1] // n_head
    groups = n_head // 2
    width = max(dqk, dv)
    state = (heads * dqk, dv)
    vmem = pl.BlockSpec(memory_space=pltpu.VMEM)
    dma = pltpu.SemaphoreType.DMA
    hbm = pl.BlockSpec(memory_space=pltpu.HBM)
    smem = pl.BlockSpec(memory_space=pltpu.SMEM)
    kept, received, mean = pl.pallas_call(
        functools.partial(kernel, n_seq, n_head, heads, dqk, dv),
        out_shape=(
            jax.ShapeDtypeStruct((tokens, cols), BF16),
            jax.ShapeDtypeStruct((groups - 1, tokens, cols), BF16),
            jax.ShapeDtypeStruct((heads,), F32),
        ),
        in_specs=[vmem] * 2 + [hbm] * 4,
        out_specs=(hbm, hbm, smem),
        scratch_shapes=[
            pltpu.VMEM(keys.shape, BF16),
            pltpu.VMEM(values.shape, BF16),
            pltpu.VMEM(queries.shape, BF16),
            pltpu.VMEM(out_weight.shape, BF16),
            pltpu.VMEM((n_seq, 4 * heads, width), F32),
            pltpu.VMEM((n_seq + 1, heads, width), F32),
            pltpu.VMEM((n_seq + 1, heads, width), F32),
            pltpu.VMEM((tokens, heads * dqk), BF16),
            pltpu.VMEM(state, BF16),
            pltpu.VMEM(state, BF16),
            pltpu.VMEM(state, BF16),
            pltpu.VMEM(state, BF16),
            pltpu.VMEM(state, BF16),
            pltpu.VMEM((tokens, heads * dv), F32),
            pltpu.VMEM((heads, tokens, 384), F32),
            pltpu.VMEM((tokens, heads * dv), BF16),
            pltpu.VMEM((groups, tokens, cols), BF16),
            pltpu.VMEM((groups, tokens, cols), BF16),
            pltpu.VMEM((groups - 1, tokens, cols), BF16),
            pltpu.VMEM((tokens, cols), BF16),
            dma((3,)),
            dma,
            dma((n_seq,)),
            dma((n_seq,)),
            dma((STATE_CHUNKS,)),
            dma((STATE_CHUNKS,)),
            dma((STATE_CHUNKS,)),
            dma((STATE_CHUNKS,)),
            dma((groups, ROW_CHUNKS)),
            dma((groups, ROW_CHUNKS)),
            dma((groups - 1, ROW_CHUNKS)),
            dma((groups - 1, ROW_CHUNKS)),
            dma((ROW_CHUNKS,)),
        ],
        compiler_params=pltpu.CompilerParams(
            collective_id=0, has_side_effects=True, vmem_limit_bytes=62 * 1024 * 1024
        ),
    )(forget_gate.T, input_gate.T, keys, values, queries, out_weight)
    span = tokens // TAIL_CHUNKS
    mixed, mean = pl.pallas_call(
        finish,
        grid=(TAIL_CHUNKS,),
        out_shape=(
            jax.ShapeDtypeStruct((tokens, cols), BF16),
            jax.ShapeDtypeStruct((heads,), F32),
        ),
        in_specs=[
            pl.BlockSpec((span, cols), lambda i: (i, 0)),
            pl.BlockSpec((groups - 1, span, cols), lambda i: (0, i, 0)),
            smem,
        ],
        out_specs=(pl.BlockSpec((span, cols), lambda i: (i, 0)), smem),
        compiler_params=pltpu.CompilerParams(vmem_limit_bytes=62 * 1024 * 1024),
    )(kept, received, mean)
    return mixed, mean


def solution(mesh):
    placed = (
        P("seq", "head"),
        P("seq", "head"),
        P("seq", "head"),
        P("seq", "head"),
        P("seq", "head"),
        P("head", None),
    )
    return jax.shard_map(
        functools.partial(shards, mesh.shape["seq"], mesh.shape["head"]),
        mesh=mesh,
        in_specs=placed,
        out_specs=(P("seq", "head"), P("head")),
        check_vma=False,
    )
```
